16 devices in a mesh: dp: 4 (over y, z, core), tp: 4 (over x).
Axes of the slice: x: 4, y: 2, z: 1, core: 2. Of those that a mesh axis runs over, the one named last changes fastest.
The devices are a block of a 4x4x8 slice.
Arguments:
- x: bfloat16 [2048, 14336], P(('dp', 'tp')), parts along dimension 0
- gain: bfloat16 [14336], replicated
- wq: bfloat16 [14336, 14336], P(None, 'tp')
- wk: bfloat16 [14336, 14336], P(None, 'tp')
- wv: bfloat16 [14336, 14336], P(None, 'tp')
- wo: bfloat16 [14336, 14336], P('tp')
Outputs:
- output: bfloat16 [2048, 14336], P(('dp', 'tp')), parts along dimension 0
There are 4 independent parts. The reference program is written for one: setup_inputs(seed, part) draws one part's arguments, and reference() takes and returns one part's arrays. A program takes and returns all parts, laid end to end along the dimension named above; an argument that names none is the same for every part.
All inputs are finite; a program needn't handle non-finite values.
Results may differ from the reference program's by a relative error of at most 0.012.
Values are sent between devices in bfloat16 or wider.
A program may use at most 768 MiB of HBM per device.

```python
import jax
import jax.numpy as jnp
from jax import lax

ROWS = 512
D = 14336
HEADS = 112
KV_HEADS = 112
HEAD = 128
THETA = 10000


def setup_inputs(seed: int = 0, part: int = 0) -> dict:
    kx, kn, kq, kk, kv, ko = jax.random.split(jax.random.key(seed), 6)

    def weights(key, rows, columns):
        return jax.random.normal(key, (rows, columns), jnp.float32) * rows**-0.5

    drawn = {
        "x": jax.random.normal(jax.random.fold_in(kx, part), (ROWS, D), jnp.float32),
        "gain": 1 + 0.1 * jax.random.normal(kn, (D,), jnp.float32),
        "wq": 2 * weights(kq, D, HEADS * HEAD),
        "wk": 2 * weights(kk, D, KV_HEADS * HEAD),
        "wv": 4 * weights(kv, D, KV_HEADS * HEAD),
        "wo": weights(ko, HEADS * HEAD, D),
    }
    return {k: v.astype(jnp.bfloat16) for k, v in drawn.items()}


def normed(x, gain):
    wide = x.astype(jnp.float32)
    scale = lax.rsqrt(jnp.mean(wide * wide, -1, keepdims=True) + 1e-6)
    return (wide * scale * gain.astype(jnp.float32)).astype(jnp.bfloat16)


def turned(t, place, theta):
    half = t.shape[-1] // 2
    angle = place.astype(jnp.float32)[:, None] * theta ** (-jnp.arange(half, dtype=jnp.float32) / half)
    cos, sin = jnp.cos(angle)[:, None], jnp.sin(angle)[:, None]
    a, b = t[..., :half].astype(jnp.float32), t[..., half:].astype(jnp.float32)
    return jnp.concatenate([a * cos - b * sin, b * cos + a * sin], -1).astype(jnp.bfloat16)


def matmul(a, w):
    return jnp.dot(a, w, preferred_element_type=jnp.float32).astype(jnp.bfloat16)


def einsum(form, a, b):
    return jnp.einsum(form, a.astype(jnp.float32), b.astype(jnp.float32))


def attention(q, k, v):
    scores = einsum("tgsd,ugd->gstu", q, k) * q.shape[-1] ** -0.5
    token = jnp.arange(q.shape[0])
    scores = jnp.where(token[:, None] >= token, scores, -jnp.inf)
    weights = jax.nn.softmax(scores, -1).astype(jnp.bfloat16)
    return einsum("gstu,ugd->tgsd", weights, v).astype(jnp.bfloat16)


def reference(x, gain, wq, wk, wv, wo):
    a, place = normed(x, gain), jnp.arange(ROWS)
    q = turned(matmul(a, wq).reshape(ROWS, HEADS, HEAD), place, THETA).reshape(ROWS, KV_HEADS, -1, HEAD)
    k = turned(matmul(a, wk).reshape(ROWS, KV_HEADS, HEAD), place, THETA)
    v = matmul(a, wv).reshape(ROWS, KV_HEADS, HEAD)
    seen = attention(q, k, v).reshape(ROWS, HEADS * HEAD)
    return (x.astype(jnp.float32) + jnp.dot(seen, wo, preferred_element_type=jnp.float32)).astype(jnp.bfloat16)
```

```python
import functools

import jax
import jax.numpy as jnp
import numpy as np
from jax import lax
from jax.experimental import pallas as pl
from jax.experimental.pallas import tpu as pltpu
from jax.sharding import PartitionSpec as P

HEAD = 128
THETA = 10000
EPS = 1e-6
LOG2E = 1.4426950408889634
HIDDEN = -2e30
CHUNK = 512
WIDE = 512
TILE = 512
FORWARD = 2
AHEAD = 4
SLOTS = 4
LIMIT = 63 * 2**20 + 900 * 2**10
MESH = pl.DeviceIdType.MESH
F32, BF16 = jnp.float32, jnp.bfloat16


def dot(a, b):
    return jnp.dot(a, b, preferred_element_type=F32)


def neighbours(n):
    me = lax.axis_index("tp")
    return me, lax.rem(me + 1, n), lax.rem(me + n - 1, n), lax.rem(me + 2, n)


def greet(right, left):
    barrier = pltpu.get_barrier_semaphore()
    for other in (right, left):
        pl.semaphore_signal(barrier, inc=1, device_id={"tp": other}, device_id_type=MESH)
    pl.semaphore_wait(barrier, 2)


def remote(src, dst, send, recv, other):
    return pltpu.make_async_remote_copy(src_ref=src, dst_ref=dst, send_sem=send, recv_sem=recv, device_id={"tp": other}, device_id_type=MESH)


def turn(t, cos, sin):
    t = t.astype(BF16).astype(F32)
    return (t * cos + pltpu.roll(t, HEAD // 2, 1) * sin).astype(BF16)


def gather_project(n, x_ref, gain_ref, cos_ref, sin_ref, wk_ref, wv_ref, wq_ref, k_out, v_out, q_out, xb_out,
                   xg, acc_k, acc_v, acc_q, ws, scale_s, wsem, own_send, own_recv, fwd_send, fwd_recv, xsem, osem):
    me, right, left, opp = neighbours(n)
    rows, width = x_ref.shape
    nk, kc, cols = width // CHUNK, CHUNK, wk_ref.shape[1]
    half = rows // 2
    weights = (wk_ref, wv_ref, wq_ref)

    def fetch(c):
        slot = lax.rem(c, 2)
        return [pltpu.make_async_copy(w.at[pl.ds(pl.multiple_of(c * kc, kc), kc), :], ws.at[slot, i], wsem.at[slot, i])
                for i, w in enumerate(weights)]

    def own(c):
        return [remote(xg.at[c, me], xg.at[c, me], own_send.at[d, c], own_recv.at[d, c], other) for d, other in enumerate((right, left))]

    def arrival(c):
        return [remote(xg.at[c, o], xg.at[c, o], own_send.at[d, c], own_recv.at[d, c], other)
                for d, (o, other) in enumerate(((left, right), (right, left)))]

    def forward(c):
        a, b = xg.at[c, left, pl.ds(half, half)], xg.at[c, right, pl.ds(0, half)]
        return [remote(a, a, fwd_send.at[0, c], fwd_recv.at[0, c], right), remote(b, b, fwd_send.at[1, c], fwd_recv.at[1, c], left)]

    def far(c):
        a, b = xg.at[c, opp, pl.ds(half, half)], xg.at[c, opp, pl.ds(0, half)]
        return [remote(a, a, fwd_send.at[0, c], fwd_recv.at[0, c], right), remote(b, b, fwd_send.at[1, c], fwd_recv.at[1, c], left)]

    def second(c):
        return pltpu.make_async_copy(xg.at[c, :, pl.ds(half, half), :], xb_out.at[c], xsem.at[lax.rem(c, 2)])

    def norm(c):
        here = pl.ds(pl.multiple_of(c * kc, kc), kc)
        wide = x_ref[:, here].astype(F32)
        xg[c, me] = (wide * scale_s[:, :1] * gain_ref[:, here].astype(F32)).astype(BF16)

    def start(copies):
        for copy in copies:
            copy.start()

    def received(copies):
        for copy in copies:
            copy.wait_recv()

    start(fetch(0))

    def squares(c, total):
        wide = x_ref[:, pl.ds(pl.multiple_of(c * kc, kc), kc)].astype(F32)
        wide = wide * wide
        for i in range(0, kc, 128):
            total = total + wide[:, i : i + 128]
        return total

    total = lax.fori_loop(0, nk, squares, jnp.zeros((rows, 128), F32))
    scale_s[...] = jnp.broadcast_to(lax.rsqrt(total.sum(-1, keepdims=True) * (1 / width) + EPS), (rows, 128))
    for c in range(AHEAD + 1):
        norm(c)
    greet(right, left)
    start(own(0))
    start(own(1))
    acc_k[...] = jnp.zeros_like(acc_k)
    acc_v[...] = jnp.zeros_like(acc_v)
    acc_q[...] = jnp.zeros_like(acc_q)
    for c in range(FORWARD):
        received(arrival(c))
        start(forward(c))
        start(own(c + 2))

    def step(c, _):
        slot = lax.rem(c, 2)

        @pl.when(c + 1 < nk)
        def _():
            start(fetch(c + 1))

        @pl.when(c + FORWARD < nk)
        def _():
            received(arrival(c + FORWARD))
            start(forward(c + FORWARD))

        @pl.when(c + AHEAD < nk)
        def _():
            start(own(c + AHEAD))

        @pl.when(c + AHEAD + 1 < nk)
        def _():
            norm(c + AHEAD + 1)

        @pl.when(c >= 2)
        def _():
            second(c - 2).wait()

        received(far(c))
        start([second(c)])
        for copy in fetch(c):
            copy.wait()
        a = xg[c].reshape(n * rows, kc)
        b = xg[c, :, :half, :].reshape(n * half, kc)
        for i in range(0, cols, WIDE):
            acc_k[:, i : i + WIDE] += dot(a, ws[slot, 0, :, i : i + WIDE])
        for i in range(0, cols, WIDE):
            acc_v[:, i : i + WIDE] += dot(a, ws[slot, 1, :, i : i + WIDE])
        for i in range(0, cols, WIDE):
            acc_q[:, i : i + WIDE] += dot(b, ws[slot, 2, :, i : i + WIDE])
        for copy in (*own(c), *forward(c)):
            copy.wait_send()
        return 0

    lax.fori_loop(0, nk, step, 0)

    group = 4 * HEAD

    def out(g):
        here = pl.ds(pl.multiple_of(g * group, group), group)
        return [pltpu.make_async_copy(ws.at[0, 0, :, here], k_out.at[:, here], osem.at[0, g]),
                pltpu.make_async_copy(ws.at[0, 1, :, here], v_out.at[:, here], osem.at[1, g]),
                pltpu.make_async_copy(ws.at[0, 2, pl.ds(0, n * half), here], q_out.at[:, here], osem.at[2, g])]

    def finish(g, _):
        here = pl.ds(pl.multiple_of(g * group, group), group)
        cos, sin = cos_ref[...].reshape(n * rows, HEAD), sin_ref[...].reshape(n * rows, HEAD)
        cos_q, sin_q = cos_ref[:, :half, :].reshape(n * half, HEAD), sin_ref[:, :half, :].reshape(n * half, HEAD)
        ws[0, 1, :, here] = acc_v[:, here].astype(BF16)
        for h in range(group // HEAD):
            at = pl.ds(pl.multiple_of(g * group + h * HEAD, HEAD), HEAD)
            ws[0, 0, :, at] = turn(acc_k[:, at], cos, sin)
            ws[0, 2, : n * half, at] = turn(acc_q[:, at], cos_q, sin_q)
        start(out(g))
        return 0

    lax.fori_loop(0, cols // group, finish, 0)
    second(nk - 2).wait()
    second(nk - 1).wait()

    def drain(g, _):
        for copy in out(g):
            copy.wait()
        return 0

    lax.fori_loop(0, cols // group, drain, 0)


def attend_scatter(n, x_ref, q_ref, k_ref, v_ref, xb_ref, cos_ref, sin_ref, wq_ref, wo_ref, y_ref,
                   qs, ks, vs, att, xb, ring, acc, opp_b, out_r, out_l, add_r, add_l, own, half_l, half_r, full_l, full_r, xy,
                   rsem, insem, xbsem, xysem, ysem, hs_sem, hr_sem, fs_sem, fr_sem, free_r, free_l):
    me, right, left, opp = neighbours(n)
    width = wo_ref.shape[1]
    cols = wq_ref.shape[1]
    nt = width // TILE
    half = x_ref.shape[0] // 2
    part = half // 2
    parts = width // cols
    nq = (cols // TILE) * parts
    nkc, kc = xb_ref.shape[0], xb_ref.shape[3]
    group = 4 * HEAD
    tokens = k_ref.shape[0]

    def start(copies):
        for copy in copies:
            copy.start()

    def tile(t):
        return pl.ds(pl.multiple_of(t * TILE, TILE), TILE)

    def wo_tile(t, slot):
        return pltpu.make_async_copy(wo_ref.at[:, tile(t)], ring.at[slot], rsem.at[slot])

    def wq_tile(u, slot):
        p, j = lax.rem(u, parts), lax.div(u, parts)
        return pltpu.make_async_copy(wq_ref.at[pl.ds(pl.multiple_of(p * cols, cols), cols), tile(j)], ring.at[slot], rsem.at[slot])

    def fetch(u):
        slot = lax.rem(u, SLOTS)

        @pl.when(u < nt)
        def _():
            wo_tile(u, slot).start()

        @pl.when((u >= nt) & (u < nt + nq))
        def _():
            wq_tile(u - nt, slot).start()

        @pl.when((u >= nt + nq) & (u < 2 * nt + nq))
        def _():
            wo_tile(u - nt - nq, slot).start()

    def arrived(u):
        slot = lax.rem(u, SLOTS)
        wo_tile(0, slot).wait()
        return slot

    def inputs(g):
        here = pl.ds(pl.multiple_of(g * group, group), group)
        return [pltpu.make_async_copy(q_ref.at[:, here], qs.at[:, here], insem.at[0, g]),
                pltpu.make_async_copy(k_ref.at[:, here], ks.at[:, here], insem.at[1, g]),
                pltpu.make_async_copy(v_ref.at[:, here], vs.at[:, here], insem.at[2, g])]

    def rows_b(c):
        per = cols // kc
        return pltpu.make_async_copy(xb_ref.at[c], xb.at[lax.div(c, per), :, :, pl.ds(pl.multiple_of(lax.rem(c, per) * kc, kc), kc)], xbsem.at[c])

    def residual(h):
        return pltpu.make_async_copy(x_ref.at[pl.ds(h * half, half), :], xy.at[h], xysem.at[h])

    def result(h, t):
        return pltpu.make_async_copy(xy.at[h, :, tile(t)], y_ref.at[pl.ds(h * half, half), tile(t)], ysem.at[h, t])

    def halves(t):
        return [remote(opp_b.at[t, pl.ds(0, part)], half_l.at[t], hs_sem.at[0, t], hr_sem.at[0, t], right),
                remote(opp_b.at[t, pl.ds(part, part)], half_r.at[t], hs_sem.at[1, t], hr_sem.at[1, t], left)]

    def blocks(t):
        return [remote(out_r.at[t], full_l.at[t], fs_sem.at[0, t], fr_sem.at[0, t], right),
                remote(out_l.at[t], full_r.at[t], fs_sem.at[1, t], fr_sem.at[1, t], left)]

    def attention(h, heads_ready):
        scale = HEAD**-0.5 * LOG2E

        def heads(g, _):
            heads_ready(g)
            for i in range(group // HEAD):
                at = pl.ds(pl.multiple_of(g * group + i * HEAD, HEAD), HEAD)
                for s in range(n // 2):
                    seen = (s + 1) * (tokens // (n // 2))
                    q = qs[pl.ds(s * 2 * half, 2 * half), at]
                    score = lax.dot_general(q, ks[:seen, at], (((1,), (1,)), ((), ())), preferred_element_type=F32)
                    row = lax.broadcasted_iota(jnp.int32, score.shape, 0)
                    place = (2 * s) * 2 * half + h * half + row + jnp.where(row >= half, half, 0)
                    score = jnp.where(lax.broadcasted_iota(jnp.int32, score.shape, 1) <= place, score, HIDDEN)
                    top = score.max(-1, keepdims=True)
                    weight = jnp.exp2((score - top) * scale)
                    total = weight.sum(-1, keepdims=True)
                    o = (dot(weight.astype(BF16), vs[:seen, at]) * (1 / total)).astype(BF16)
                    for j in range(2):
                        att[lax.rem(2 * s + j + n - me, n), :, at] = o[j * half : (j + 1) * half]
            return 0

        lax.fori_loop(0, cols // group, heads, 0)

    def term(t, slot):
        got = dot(att[...].reshape(n * half, cols), ring[slot])
        own[t] = got[:half]
        add_r[t] = got[half : half + part]
        out_r[t, part:] = got[half + part : 2 * half].astype(BF16)
        opp_b[t] = got[2 * half : 3 * half].astype(BF16)
        out_l[t, :part] = got[3 * half : 3 * half + part].astype(BF16)
        add_l[t] = got[3 * half + part :]

    def add(t):
        for copy in halves(t):
            copy.wait_recv()
        out_r[t, :part] = (add_r[t] + half_l[t].astype(F32)).astype(BF16)
        out_l[t, part:] = (add_l[t] + half_r[t].astype(F32)).astype(BF16)

    def close(h, t):
        for copy in blocks(t):
            copy.wait_recv()
        here = tile(t)
        xy[h, :, here] = (xy[h, :, here].astype(F32) + (own[t] + full_l[t].astype(F32) + full_r[t].astype(F32))).astype(BF16)
        result(h, t).start()

    def serve(h, s):
        odd = lax.rem(s, 2) == 1
        t = lax.div(s - 3, 2)

        @pl.when(odd & (s >= 3) & (t < nt))
        def _():
            add(t)

        @pl.when(~odd & (s >= 4) & (lax.div(s - 4, 2) < nt))
        def _():
            start(blocks(lax.div(s - 4, 2)))

        @pl.when(~odd & (s >= LAG) & (lax.div(s - LAG, 2) < nt))
        def _():
            close(h, lax.div(s - LAG, 2))

    def project(h, first):
        def unit(t, _):
            fetch(first + t + SLOTS - 1)
            slot = arrived(first + t)

            @pl.when(t >= 1)
            def _():
                start(halves(t - 1))

            serve(h, t)
            term(t, slot)
            return 0

        lax.fori_loop(0, nt, unit, 0)
        start(halves(nt - 1))

    def drain(h, s):
        added, sent, closed = (s - 2) // 2, (s - 3) // 2, max((s - LAG + 1) // 2, 0)

        def rest(t, _):
            @pl.when(t >= added)
            def _():
                add(t)

            @pl.when(t - 1 >= sent)
            def _():
                start(blocks(t - 1))
            return 0

        if sent < nt:
            lax.fori_loop(sent, nt, rest, 0)
            start(blocks(nt - 1))

        def last(t, _):
            close(h, t)
            return 0

        lax.fori_loop(closed, nt, last, 0)

        def settle(t, _):
            for copy in (*halves(t), *blocks(t)):
                copy.wait_send()
            return 0

        lax.fori_loop(0, nt, settle, 0)

    for u in range(SLOTS - 1):
        wo_tile(u, u).start()

    def begin(g, _):
        start(inputs(g))
        return 0

    lax.fori_loop(0, cols // group, begin, 0)

    def begin_b(c, _):
        rows_b(c).start()
        return 0

    lax.fori_loop(0, nkc, begin_b, 0)
    for h in range(2):
        residual(h).start()
    greet(right, left)

    def ready(g):
        for copy in inputs(g):
            copy.wait()

    attention(0, ready)
    for h in range(2):
        residual(h).wait()
    project(0, 0)

    def wait_b(c, _):
        rows_b(c).wait()
        return 0

    lax.fori_loop(0, nkc, wait_b, 0)

    def queries(j, _):
        for p in range(parts):
            u = nt + j * parts + p
            fetch(u + SLOTS - 1)
            slot = arrived(u)
            serve(0, u)
            got = dot(xb[p].reshape(n * half, cols), ring[slot])
            acc[...] = got if p == 0 else acc[...] + got
        for i in range(TILE // HEAD):
            at = pl.ds(pl.multiple_of(j * TILE + i * HEAD, HEAD), HEAD)
            qs[:, at] = turn(acc[:, i * HEAD : (i + 1) * HEAD], cos_ref[...], sin_ref[...])
        return 0

    lax.fori_loop(0, cols // TILE, queries, 0)
    attention(1, lambda g: None)
    drain(0, nt + nq)
    pl.semaphore_signal(free_r, inc=1, device_id={"tp": left}, device_id_type=MESH)
    pl.semaphore_signal(free_l, inc=1, device_id={"tp": right}, device_id_type=MESH)
    pl.semaphore_wait(free_r, 1)
    pl.semaphore_wait(free_l, 1)
    project(1, nt + nq)
    drain(1, nt)

    def written(t, _):
        for h in range(2):
            result(h, t).wait()
        return 0

    lax.fori_loop(0, nt, written, 0)


LAG = 12


def tables(tokens):
    i = HEAD // 2
    angle = np.arange(tokens, dtype=np.float32)[:, None] * np.power(np.float32(THETA), -np.arange(i, dtype=np.float32) / np.float32(i))
    cos, sin = np.cos(angle).astype(np.float32), np.sin(angle).astype(np.float32)
    return np.concatenate([cos, cos], 1), np.concatenate([-sin, sin], 1)


def solution(mesh):
    n = mesh.shape["tp"]
    anywhere = pl.BlockSpec(memory_space=pl.ANY)
    vmem = pl.BlockSpec(memory_space=pltpu.VMEM)
    dma = pltpu.SemaphoreType.DMA

    def first(x, gain, wk, wv, wq, cos, sin):
        rows, width = x.shape
        cols, nk, half = wk.shape[1], x.shape[1] // CHUNK, rows // 2
        return pl.pallas_call(
            functools.partial(gather_project, n),
            in_specs=[vmem] * 4 + [anywhere] * 3,
            out_specs=[anywhere] * 4,
            out_shape=[jax.ShapeDtypeStruct((n * rows, cols), BF16), jax.ShapeDtypeStruct((n * rows, cols), BF16),
                       jax.ShapeDtypeStruct((n * half, cols), BF16), jax.ShapeDtypeStruct((nk, n, half, CHUNK), BF16)],
            scratch_shapes=[
                pltpu.VMEM((nk, n, rows, CHUNK), BF16),
                pltpu.VMEM((n * rows, cols), F32), pltpu.VMEM((n * rows, cols), F32), pltpu.VMEM((n * half, cols), F32),
                pltpu.VMEM((2, 3, CHUNK, cols), BF16), pltpu.VMEM((rows, 128), F32),
                dma((2, 3)), dma((2, nk)), dma((2, nk)), dma((2, nk)), dma((2, nk)), dma((2,)), dma((3, cols // (4 * HEAD)))],
            compiler_params=pltpu.CompilerParams(collective_id=0, has_side_effects=True, vmem_limit_bytes=LIMIT),
            name="gather_project",
        )(x, gain[None], cos.reshape(n, rows, HEAD), sin.reshape(n, rows, HEAD), wk, wv, wq)

    def then(x, q, k, v, xb, cos, sin, wq, wo):
        rows, width = x.shape
        cols, nt, half = wq.shape[1], x.shape[1] // TILE, rows // 2
        nk, part = xb.shape[0], half // 2
        cos, sin = (a.reshape(n, 2, half, HEAD)[:, 1].reshape(n * half, HEAD) for a in (cos, sin))
        return pl.pallas_call(
            functools.partial(attend_scatter, n),
            in_specs=[anywhere] * 5 + [vmem] * 2 + [anywhere] * 2,
            out_specs=anywhere,
            out_shape=jax.ShapeDtypeStruct((rows, width), BF16),
            scratch_shapes=[
                pltpu.VMEM((n * half, cols), BF16), pltpu.VMEM((n * rows, cols), BF16), pltpu.VMEM((n * rows, cols), BF16),
                pltpu.VMEM((n, half, cols), BF16), pltpu.VMEM((width // cols, n, half, cols), BF16),
                pltpu.VMEM((SLOTS, cols, TILE), BF16), pltpu.VMEM((n * half, TILE), F32),
                pltpu.VMEM((nt, half, TILE), BF16), pltpu.VMEM((nt, half, TILE), BF16), pltpu.VMEM((nt, half, TILE), BF16),
                pltpu.VMEM((nt, part, TILE), F32), pltpu.VMEM((nt, part, TILE), F32), pltpu.VMEM((nt, half, TILE), F32),
                pltpu.VMEM((nt, part, TILE), BF16), pltpu.VMEM((nt, part, TILE), BF16),
                pltpu.VMEM((nt, half, TILE), BF16), pltpu.VMEM((nt, half, TILE), BF16),
                pltpu.VMEM((2, half, width), BF16),
                dma((SLOTS,)), dma((3, cols // (4 * HEAD))), dma((nk,)), dma((2,)), dma((2, nt)),
                dma((2, nt)), dma((2, nt)), dma((2, nt)), dma((2, nt)),
                pltpu.SemaphoreType.REGULAR, pltpu.SemaphoreType.REGULAR],
            compiler_params=pltpu.CompilerParams(collective_id=1, has_side_effects=True, vmem_limit_bytes=LIMIT),
            name="attend_scatter",
        )(x, q, k, v, xb, cos, sin, wq, wo)

    def step(x, gain, wq, wk, wv, wo):
        cos, sin = tables(n * x.shape[0])
        k, v, q, xb = first(x, gain, wk, wv, wq, cos, sin)
        return then(x, q, k, v, xb, cos, sin, wq, wo)

    tokens, columns = P(("dp", "tp"), None), P(None, "tp")
    return jax.shard_map(
        step,
        mesh=mesh,
        in_specs=(tokens, P(None), columns, columns, columns, P("tp", None)),
        out_specs=tokens,
        check_vma=False,
    )
```

```python
import functools

import jax
import jax.numpy as jnp
import numpy as np
from jax import lax
from jax.experimental import pallas as pl
from jax.experimental.pallas import tpu as pltpu
from jax.sharding import PartitionSpec as P

HEAD = 128
THETA = 10000
EPS = 1e-6
LOG2E = 1.4426950408889634
HIDDEN = -2e30
CHUNK = 512
WIDE = 512
TILE = 512
FORWARD = 1
AHEAD = 3
SLOTS = 5
LIMIT = 63 * 2**20 + 900 * 2**10
MESH = pl.DeviceIdType.MESH
F32, BF16 = jnp.float32, jnp.bfloat16


def dot(a, b):
    return jnp.dot(a, b, preferred_element_type=F32)


def neighbours(n):
    me = lax.axis_index("tp")
    return me, lax.rem(me + 1, n), lax.rem(me + n - 1, n), lax.rem(me + 2, n)


def greet(right, left):
    barrier = pltpu.get_barrier_semaphore()
    for other in (right, left):
        pl.semaphore_signal(barrier, inc=1, device_id={"tp": other}, device_id_type=MESH)
    return lambda: pl.semaphore_wait(barrier, 2)


def remote(src, dst, send, recv, other):
    return pltpu.make_async_remote_copy(src_ref=src, dst_ref=dst, send_sem=send, recv_sem=recv, device_id={"tp": other}, device_id_type=MESH)


def turn(t, cos, sin):
    t = t.astype(BF16).astype(F32)
    return (t * cos + pltpu.roll(t, HEAD // 2, 1) * sin).astype(BF16)


def gather_project(n, x_ref, gain_ref, cos_ref, sin_ref, wk_ref, wv_ref, wq_ref, k_out, v_out, q_out, xb_out,
                   xg, acc_k, acc_v, acc_q, ws, scale_s, wsem, first_recv, own_send, own_recv, fwd_send, fwd_recv, xsem, osem):
    me, right, left, opp = neighbours(n)
    rows, width = x_ref.shape
    nk, kc, cols = width // CHUNK, CHUNK, wk_ref.shape[1]
    half = rows // 2
    weights = (wk_ref, wv_ref, wq_ref)

    def fetch(c):
        slot = lax.rem(c, 2)
        return [pltpu.make_async_copy(w.at[pl.ds(pl.multiple_of(c * kc, kc), kc), :], ws.at[slot, i], wsem.at[slot, i])
                for i, w in enumerate(weights)]

    def own(c):
        return [remote(xg.at[c, me], xg.at[c, me], own_send.at[d, c], own_recv.at[d, c], other) for d, other in enumerate((right, left))]

    def arrival(c):
        return [remote(xg.at[c, o], xg.at[c, o], own_send.at[d, c], own_recv.at[d, c], other)
                for d, (o, other) in enumerate(((left, right), (right, left)))]

    def forward(c):
        a, b = xg.at[c, left, pl.ds(half, half)], xg.at[c, right, pl.ds(0, half)]
        return [remote(a, a, fwd_send.at[0, c], fwd_recv.at[0, c], right), remote(b, b, fwd_send.at[1, c], fwd_recv.at[1, c], left)]

    def far(c):
        a, b = xg.at[c, opp, pl.ds(half, half)], xg.at[c, opp, pl.ds(0, half)]
        return [remote(a, a, fwd_send.at[0, c], fwd_recv.at[0, c], right), remote(b, b, fwd_send.at[1, c], fwd_recv.at[1, c], left)]

    def second(c):
        return pltpu.make_async_copy(xg.at[c, :, pl.ds(half, half), :], xb_out.at[c], xsem.at[lax.rem(c, 2)])

    def norm(c):
        here = pl.ds(pl.multiple_of(c * kc, kc), kc)
        wide = x_ref[:, here].astype(F32)
        xg[c, me] = (wide * scale_s[:, :1] * gain_ref[here].astype(F32)[None]).astype(BF16)

    def start(copies):
        for copy in copies:
            copy.start()

    def received(copies):
        for copy in copies:
            copy.wait_recv()

    greeted = greet(right, left)
    start(fetch(0))

    def squares(c, total):
        wide = x_ref[:, pl.ds(pl.multiple_of(c * kc, kc), kc)].astype(F32)
        wide = wide * wide
        for i in range(0, kc, 128):
            total = total + wide[:, i : i + 128]
        return total

    total = lax.fori_loop(0, nk, squares, jnp.zeros((rows, 128), F32))
    scale_s[...] = jnp.broadcast_to(lax.rsqrt(total.sum(-1, keepdims=True) * (1 / width) + EPS), (rows, 128))
    norm(0)
    norm(1)
    greeted()
    for there, sems in ((0, first_recv), (1, own_recv.at[:, 0])):
        for d, other in enumerate((right, left)):
            at = xg.at[0, me, pl.ds(half * ((there + d + 1) % 2), half)]
            remote(at, at, own_send.at[d, 0], sems.at[d], other).start()
    for c in range(2, AHEAD + 1):
        norm(c)
    acc_k[...] = jnp.zeros_like(acc_k)
    acc_v[...] = jnp.zeros_like(acc_v)
    acc_q[...] = jnp.zeros_like(acc_q)
    for d, (o, other) in enumerate(((left, right), (right, left))):
        at = xg.at[0, o, pl.ds(half * (1 - d), half)]
        remote(at, at, own_send.at[d, 0], first_recv.at[d], other).wait_recv()
    start(forward(0))
    start(own(1))
    for d, (o, other) in enumerate(((left, right), (right, left))):
        at = xg.at[0, o, pl.ds(half * d, half)]
        remote(at, at, own_send.at[d, 0], own_recv.at[d, 0], other).wait_recv()
    for c in range(2, AHEAD):
        start(own(c))

    def step(c, _):
        slot = lax.rem(c, 2)

        @pl.when(c + 1 < nk)
        def _():
            start(fetch(c + 1))

        @pl.when(c + FORWARD < nk)
        def _():
            received(arrival(c + FORWARD))
            start(forward(c + FORWARD))

        @pl.when(c + AHEAD < nk)
        def _():
            start(own(c + AHEAD))

        @pl.when(c + AHEAD + 1 < nk)
        def _():
            norm(c + AHEAD + 1)

        @pl.when(c >= 2)
        def _():
            second(c - 2).wait()

        received(far(c))
        start([second(c)])
        for copy in fetch(c):
            copy.wait()
        a = xg[c].reshape(n * rows, kc)
        b = xg[c, :, :half, :].reshape(n * half, kc)
        for i in range(0, cols, WIDE):
            acc_k[:, i : i + WIDE] += dot(a, ws[slot, 0, :, i : i + WIDE])
        for i in range(0, cols, WIDE):
            acc_v[:, i : i + WIDE] += dot(a, ws[slot, 1, :, i : i + WIDE])
        for i in range(0, cols, WIDE):
            acc_q[:, i : i + WIDE] += dot(b, ws[slot, 2, :, i : i + WIDE])
        for copy in (*own(c), *forward(c)):
            copy.wait_send()
        return 0

    lax.fori_loop(0, nk, step, 0)

    group = 4 * HEAD

    def out(g):
        here = pl.ds(pl.multiple_of(g * group, group), group)
        return [pltpu.make_async_copy(ws.at[0, 0, :, here], k_out.at[:, here], osem.at[0, g]),
                pltpu.make_async_copy(ws.at[0, 1, :, here], v_out.at[:, here], osem.at[1, g]),
                pltpu.make_async_copy(ws.at[0, 2, pl.ds(0, n * half), here], q_out.at[:, here], osem.at[2, g])]

    def finish(g, _):
        here = pl.ds(pl.multiple_of(g * group, group), group)
        cos, sin = cos_ref[...].reshape(n * rows, HEAD), sin_ref[...].reshape(n * rows, HEAD)
        cos_q, sin_q = cos_ref[:, :half, :].reshape(n * half, HEAD), sin_ref[:, :half, :].reshape(n * half, HEAD)
        ws[0, 1, :, here] = acc_v[:, here].astype(BF16)
        for h in range(group // HEAD):
            at = pl.ds(pl.multiple_of(g * group + h * HEAD, HEAD), HEAD)
            ws[0, 0, :, at] = turn(acc_k[:, at], cos, sin)
            ws[0, 2, : n * half, at] = turn(acc_q[:, at], cos_q, sin_q)
        start(out(g))
        return 0

    lax.fori_loop(0, cols // group, finish, 0)
    second(nk - 2).wait()
    second(nk - 1).wait()

    def drain(g, _):
        for copy in out(g):
            copy.wait()
        return 0

    lax.fori_loop(0, cols // group, drain, 0)


def attend_scatter(n, x_ref, q_ref, k_ref, v_ref, xb_ref, cos_ref, sin_ref, wq_ref, wo_ref, y_ref,
                   qs, ks, vs, att, xb, ring, acc, opp_b, out_r, out_l, add_r, add_l, own, half_l, half_r, full_l, full_r, xy,
                   rsem, insem, xbsem, xysem, ysem, hs_sem, hr_sem, fs_sem, fr_sem, free_r, free_l):
    me, right, left, opp = neighbours(n)
    width = wo_ref.shape[1]
    cols = wq_ref.shape[1]
    nt = width // TILE
    half = x_ref.shape[0] // 2
    part = half // 2
    parts = width // cols
    nq = (cols // TILE) * parts
    nkc, kc = xb_ref.shape[0], xb_ref.shape[3]
    group = 4 * HEAD
    tokens = k_ref.shape[0]

    def start(copies):
        for copy in copies:
            copy.start()

    def tile(t):
        return pl.ds(pl.multiple_of(t * TILE, TILE), TILE)

    def wo_tile(t, slot):
        return pltpu.make_async_copy(wo_ref.at[:, tile(t)], ring.at[slot], rsem.at[slot])

    def wq_tile(u, slot):
        p, j = lax.rem(u, parts), lax.div(u, parts)
        return pltpu.make_async_copy(wq_ref.at[pl.ds(pl.multiple_of(p * cols, cols), cols), tile(j)], ring.at[slot], rsem.at[slot])

    def fetch(u):
        slot = lax.rem(u, SLOTS)

        @pl.when(u < nt)
        def _():
            wo_tile(u, slot).start()

        @pl.when((u >= nt) & (u < nt + nq))
        def _():
            wq_tile(u - nt, slot).start()

        @pl.when((u >= nt + nq) & (u < 2 * nt + nq))
        def _():
            wo_tile(u - nt - nq, slot).start()

    def arrived(u):
        slot = lax.rem(u, SLOTS)
        wo_tile(0, slot).wait()
        return slot

    def inputs(g):
        here = pl.ds(pl.multiple_of(g * group, group), group)
        return [pltpu.make_async_copy(q_ref.at[:, here], qs.at[:, here], insem.at[0, g]),
                pltpu.make_async_copy(k_ref.at[:, here], ks.at[:, here], insem.at[1, g]),
                pltpu.make_async_copy(v_ref.at[:, here], vs.at[:, here], insem.at[2, g])]

    def rows_b(c):
        per = cols // kc
        return pltpu.make_async_copy(xb_ref.at[c], xb.at[lax.div(c, per), :, :, pl.ds(pl.multiple_of(lax.rem(c, per) * kc, kc), kc)], xbsem.at[c])

    def residual(h):
        return pltpu.make_async_copy(x_ref.at[pl.ds(h * half, half), :], xy.at[h], xysem.at[h])

    def result(h, t):
        return pltpu.make_async_copy(xy.at[h, :, tile(t)], y_ref.at[pl.ds(h * half, half), tile(t)], ysem.at[h, t])

    def halves(t):
        return [remote(opp_b.at[t, pl.ds(0, part)], half_l.at[t], hs_sem.at[0, t], hr_sem.at[0, t], right),
                remote(opp_b.at[t, pl.ds(part, part)], half_r.at[t], hs_sem.at[1, t], hr_sem.at[1, t], left)]

    def blocks(t):
        return [remote(out_r.at[t], full_l.at[t], fs_sem.at[0, t], fr_sem.at[0, t], right),
                remote(out_l.at[t], full_r.at[t], fs_sem.at[1, t], fr_sem.at[1, t], left)]

    def attention(h, heads_ready):
        scale = HEAD**-0.5 * LOG2E

        def heads(g, _):
            heads_ready(g)
            for i in range(group // HEAD):
                at = pl.ds(pl.multiple_of(g * group + i * HEAD, HEAD), HEAD)
                for s in range(n // 2):
                    seen = (s + 1) * (tokens // (n // 2))
                    q = qs[pl.ds(s * 2 * half, 2 * half), at]
                    score = lax.dot_general(q, ks[:seen, at], (((1,), (1,)), ((), ())), preferred_element_type=F32)
                    row = lax.broadcasted_iota(jnp.int32, score.shape, 0)
                    place = (2 * s) * 2 * half + h * half + row + jnp.where(row >= half, half, 0)
                    score = jnp.where(lax.broadcasted_iota(jnp.int32, score.shape, 1) <= place, score, HIDDEN)
                    top = score.max(-1, keepdims=True)
                    weight = jnp.exp2((score - top) * scale)
                    got = dot(weight.astype(BF16), jnp.concatenate([vs[:seen, at], jnp.ones((seen, HEAD), BF16)], 1))
                    o = (got[:, :HEAD] / got[:, HEAD:]).astype(BF16)
                    for j in range(2):
                        att[lax.rem(2 * s + j + n - me, n), :, at] = o[j * half : (j + 1) * half]
            return 0

        lax.fori_loop(0, cols // group, heads, 0)

    def term(t, slot):
        got = dot(att[...].reshape(n * half, cols), ring[slot])
        own[t] = got[:half]
        add_r[t] = got[half : half + part]
        out_r[t, part:] = got[half + part : 2 * half].astype(BF16)
        opp_b[t] = got[2 * half : 3 * half].astype(BF16)
        out_l[t, :part] = got[3 * half : 3 * half + part].astype(BF16)
        add_l[t] = got[3 * half + part :]

    def add(t):
        for copy in halves(t):
            copy.wait_recv()
        out_r[t, :part] = (add_r[t] + half_l[t].astype(F32)).astype(BF16)
        out_l[t, part:] = (add_l[t] + half_r[t].astype(F32)).astype(BF16)

    def close(h, t):
        for copy in blocks(t):
            copy.wait_recv()
        here = tile(t)
        xy[h, :, here] = (xy[h, :, here].astype(F32) + (own[t] + full_l[t].astype(F32) + full_r[t].astype(F32))).astype(BF16)
        result(h, t).start()

    def serve(h, i):
        @pl.when((i >= 3) & (i - 3 < nt))
        def _():
            start(blocks(i - 3))

        @pl.when((i >= 2) & (i - 2 < nt))
        def _():
            add(i - 2)

        @pl.when((i >= LAG) & (i - LAG < nt))
        def _():
            close(h, i - LAG)

    def project(h, first):
        def pair(i, _):
            fetch(first + 2 * i + SLOTS - 2)
            fetch(first + 2 * i + SLOTS - 1)

            @pl.when(i >= 1)
            def _():
                start(halves(2 * i - 2))
                start(halves(2 * i - 1))

            serve(h, i)
            slots = [arrived(first + 2 * i + j) for j in range(2)]
            for j in range(2):
                term(2 * i + j, slots[j])
            return 0

        lax.fori_loop(0, nt // 2, pair, 0)
        start(halves(nt - 2))
        start(halves(nt - 1))

    def drain(h, i):
        added, sent = min(i - 2, nt), min(i - 3, nt)

        def rest(t, _):
            @pl.when(t >= added)
            def _():
                add(t)

            @pl.when(t - 1 >= sent)
            def _():
                start(blocks(t - 1))
            return 0

        if sent < nt:
            lax.fori_loop(sent, nt, rest, 0)
            start(blocks(nt - 1))

    def finish(h, i):
        closed = min(i - LAG, nt)

        def last(t, _):
            close(h, t)
            return 0

        lax.fori_loop(closed, nt, last, 0)

        def settle(t, _):
            for copy in (*halves(t), *blocks(t)):
                copy.wait_send()
            return 0

        lax.fori_loop(0, nt, settle, 0)

    greeted = greet(right, left)

    def begin(g, _):
        start(inputs(g))
        return 0

    lax.fori_loop(0, cols // group, begin, 0)

    for u in range(SLOTS - 2):
        wo_tile(u, u).start()

    def begin_b(c, _):
        rows_b(c).start()
        return 0

    lax.fori_loop(0, nkc, begin_b, 0)
    for h in range(2):
        residual(h).start()

    def ready(g):
        for copy in inputs(g):
            copy.wait()

    attention(0, ready)
    for h in range(2):
        residual(h).wait()
    greeted()
    project(0, 0)

    def wait_b(c, _):
        rows_b(c).wait()
        return 0

    lax.fori_loop(0, nkc, wait_b, 0)

    def queries(j, _):
        for p in range(0, parts, 2):
            u = nt + j * parts + p
            fetch(u + SLOTS - 2)
            fetch(u + SLOTS - 1)
            serve(0, lax.div(u, 2))
            slots = [arrived(u + i) for i in range(2)]
            got = dot(xb[p].reshape(n * half, cols), ring[slots[0]]) + dot(xb[p + 1].reshape(n * half, cols), ring[slots[1]])
            acc[...] = got if p == 0 else acc[...] + got
        for i in range(TILE // HEAD):
            at = pl.ds(pl.multiple_of(j * TILE + i * HEAD, HEAD), HEAD)
            qs[:, at] = turn(acc[:, i * HEAD : (i + 1) * HEAD], cos_ref[...], sin_ref[...])
        return 0

    lax.fori_loop(0, cols // TILE, queries, 0)
    drain(0, (nt + nq) // 2)
    attention(1, lambda g: None)
    finish(0, (nt + nq) // 2)
    pl.semaphore_signal(free_r, inc=1, device_id={"tp": left}, device_id_type=MESH)
    pl.semaphore_signal(free_l, inc=1, device_id={"tp": right}, device_id_type=MESH)
    pl.semaphore_wait(free_r, 1)
    pl.semaphore_wait(free_l, 1)
    project(1, nt + nq)
    drain(1, nt // 2)
    finish(1, nt // 2)

    def written(t, _):
        for h in range(2):
            result(h, t).wait()
        return 0

    lax.fori_loop(0, nt, written, 0)


LAG = 7


def tables(tokens):
    i = HEAD // 2
    angle = np.arange(tokens, dtype=np.float32)[:, None] * np.power(np.float32(THETA), -np.arange(i, dtype=np.float32) / np.float32(i))
    cos, sin = np.cos(angle).astype(np.float32), np.sin(angle).astype(np.float32)
    return np.concatenate([cos, cos], 1), np.concatenate([-sin, sin], 1)


def solution(mesh):
    n = mesh.shape["tp"]
    anywhere = pl.BlockSpec(memory_space=pl.ANY)
    vmem = pl.BlockSpec(memory_space=pltpu.VMEM)
    dma = pltpu.SemaphoreType.DMA

    def first(x, gain, wk, wv, wq, cos, sin):
        rows, width = x.shape
        cols, nk, half = wk.shape[1], x.shape[1] // CHUNK, rows // 2
        return pl.pallas_call(
            functools.partial(gather_project, n),
            in_specs=[vmem] * 4 + [anywhere] * 3,
            out_specs=[anywhere] * 4,
            out_shape=[jax.ShapeDtypeStruct((n * rows, cols), BF16), jax.ShapeDtypeStruct((n * rows, cols), BF16),
                       jax.ShapeDtypeStruct((n * half, cols), BF16), jax.ShapeDtypeStruct((nk, n, half, CHUNK), BF16)],
            scratch_shapes=[
                pltpu.VMEM((nk, n, rows, CHUNK), BF16),
                pltpu.VMEM((n * rows, cols), F32), pltpu.VMEM((n * rows, cols), F32), pltpu.VMEM((n * half, cols), F32),
                pltpu.VMEM((2, 3, CHUNK, cols), BF16), pltpu.VMEM((rows, 128), F32),
                dma((2, 3)), dma((2,)), dma((2, nk)), dma((2, nk)), dma((2, nk)), dma((2, nk)), dma((2,)), dma((3, cols // (4 * HEAD)))],
            compiler_params=pltpu.CompilerParams(collective_id=0, has_side_effects=True, vmem_limit_bytes=LIMIT),
            name="gather_project",
        )(x, gain, cos.reshape(n, rows, HEAD), sin.reshape(n, rows, HEAD), wk, wv, wq)

    def then(x, q, k, v, xb, cos, sin, wq, wo):
        rows, width = x.shape
        cols, nt, half = wq.shape[1], x.shape[1] // TILE, rows // 2
        nk, part = xb.shape[0], half // 2
        cos, sin = (a.reshape(n, 2, half, HEAD)[:, 1].reshape(n * half, HEAD) for a in (cos, sin))
        return pl.pallas_call(
            functools.partial(attend_scatter, n),
            in_specs=[anywhere] * 5 + [vmem] * 2 + [anywhere] * 2,
            out_specs=anywhere,
            out_shape=jax.ShapeDtypeStruct((rows, width), BF16),
            scratch_shapes=[
                pltpu.VMEM((n * half, cols), BF16), pltpu.VMEM((n * rows, cols), BF16), pltpu.VMEM((n * rows, cols), BF16),
                pltpu.VMEM((n, half, cols), BF16), pltpu.VMEM((width // cols, n, half, cols), BF16),
                pltpu.VMEM((SLOTS, cols, TILE), BF16), pltpu.VMEM((n * half, TILE), F32),
                pltpu.VMEM((nt, half, TILE), BF16), pltpu.VMEM((nt, half, TILE), BF16), pltpu.VMEM((nt, half, TILE), BF16),
                pltpu.VMEM((nt, part, TILE), F32), pltpu.VMEM((nt, part, TILE), F32), pltpu.VMEM((nt, half, TILE), F32),
                pltpu.VMEM((nt, part, TILE), BF16), pltpu.VMEM((nt, part, TILE), BF16),
                pltpu.VMEM((nt, half, TILE), BF16), pltpu.VMEM((nt, half, TILE), BF16),
                pltpu.VMEM((2, half, width), BF16),
                dma((SLOTS,)), dma((3, cols // (4 * HEAD))), dma((nk,)), dma((2,)), dma((2, nt)),
                dma((2, nt)), dma((2, nt)), dma((2, nt)), dma((2, nt)),
                pltpu.SemaphoreType.REGULAR, pltpu.SemaphoreType.REGULAR],
            compiler_params=pltpu.CompilerParams(collective_id=1, has_side_effects=True, vmem_limit_bytes=LIMIT),
            name="attend_scatter",
        )(x, q, k, v, xb, cos, sin, wq, wo)

    def step(x, gain, wq, wk, wv, wo):
        cos, sin = tables(n * x.shape[0])
        k, v, q, xb = first(x, gain, wk, wv, wq, cos, sin)
        return then(x, q, k, v, xb, cos, sin, wq, wo)

    tokens, columns = P(("dp", "tp"), None), P(None, "tp")
    return jax.shard_map(
        step,
        mesh=mesh,
        in_specs=(tokens, P(None), columns, columns, columns, P("tp", None)),
        out_specs=tokens,
        check_vma=False,
    )
```

```python
import functools

import jax
import jax.numpy as jnp
import numpy as np
from jax import lax
from jax.experimental import pallas as pl
from jax.experimental.pallas import tpu as pltpu
from jax.sharding import PartitionSpec as P

HEAD = 128
THETA = 10000
EPS = 1e-6
LOG2E = 1.4426950408889634
HIDDEN = -2e30
CHUNK = 512
WIDE = 512
TILE = 512
AHEAD = 3
SLOTS = 5
LIMIT = 63 * 2**20 + 900 * 2**10
MESH = pl.DeviceIdType.MESH
F32, BF16 = jnp.float32, jnp.bfloat16


def dot(a, b):
    return jnp.dot(a, b, preferred_element_type=F32)


def neighbours(n):
    me = lax.axis_index("tp")
    return me, lax.rem(me + 1, n), lax.rem(me + n - 1, n), lax.rem(me + 2, n)


def greet(right, left):
    barrier = pltpu.get_barrier_semaphore()
    for other in (right, left):
        pl.semaphore_signal(barrier, inc=1, device_id={"tp": other}, device_id_type=MESH)
    return lambda: pl.semaphore_wait(barrier, 2)


def remote(src, dst, send, recv, other):
    return pltpu.make_async_remote_copy(src_ref=src, dst_ref=dst, send_sem=send, recv_sem=recv, device_id={"tp": other}, device_id_type=MESH)


def turn(t, cos, sin):
    t = t.astype(BF16).astype(F32)
    return (t * cos + pltpu.roll(t, HEAD // 2, 1) * sin).astype(BF16)


def gather_project(n, x_ref, gain_ref, cos_ref, sin_ref, wk_ref, wv_ref, wq_ref, k_out, v_out, q_out, xb_out,
                   xg, acc_k, acc_v, acc_q, ws, scale_s, wsem, first_recv, late_recv, own_send, own_recv, fwd_send, fwd_recv, xsem, osem):
    me, right, left, opp = neighbours(n)
    rows, width = x_ref.shape
    nk, kc, cols = width // CHUNK, CHUNK, wk_ref.shape[1]
    half = rows // 2
    weights = (wk_ref, wv_ref, wq_ref)

    def fetch(c):
        slot = lax.rem(c, 2)
        return [pltpu.make_async_copy(w.at[pl.ds(pl.multiple_of(c * kc, kc), kc), :], ws.at[slot, i], wsem.at[slot])
                for i, w in enumerate(weights)]

    def own(c):
        return [remote(xg.at[c, me], xg.at[c, me], own_send.at[d], own_recv.at[c], other) for d, other in enumerate((right, left))]

    def arrival(c):
        both = xg.at[c, pl.ds(0, 2)]
        return [remote(both, both, own_send.at[0], own_recv.at[c], right)]

    def forward(c):
        a, b = xg.at[c, left, pl.ds(half, half)], xg.at[c, right, pl.ds(0, half)]
        return [remote(a, a, fwd_send.at[0], fwd_recv.at[c], right), remote(b, b, fwd_send.at[1], fwd_recv.at[c], left)]

    def far(c):
        return [remote(xg.at[c, opp], xg.at[c, opp], fwd_send.at[0], fwd_recv.at[c], right)]

    def second(c):
        return pltpu.make_async_copy(xg.at[c, :, pl.ds(half, half), :], xb_out.at[c], xsem)

    def norm(c):
        here = pl.ds(pl.multiple_of(c * kc, kc), kc)
        wide = x_ref[:, here].astype(F32)
        xg[c, me] = (wide * scale_s[:, :1] * gain_ref[here].astype(F32)[None]).astype(BF16)

    def start(copies):
        for copy in copies:
            copy.start()

    def received(copies):
        for copy in copies:
            copy.wait_recv()

    greeted = greet(right, left)
    start(fetch(0))

    def squares(c, total):
        wide = x_ref[:, pl.ds(pl.multiple_of(c * kc, kc), kc)].astype(F32)
        wide = wide * wide
        for i in range(0, kc, 128):
            total = total + wide[:, i : i + 128]
        return total

    total = lax.fori_loop(0, nk, squares, jnp.zeros((rows, 128), F32))
    scale_s[...] = jnp.broadcast_to(lax.rsqrt(total.sum(-1, keepdims=True) * (1 / width) + EPS), (rows, 128))
    norm(0)
    norm(1)
    greeted()
    for there, sems in ((0, first_recv), (1, late_recv)):
        for d, other in enumerate((right, left)):
            at = xg.at[0, me, pl.ds(half * ((there + d + 1) % 2), half)]
            remote(at, at, own_send.at[d], sems.at[d], other).start()
    for c in range(2, AHEAD + 1):
        norm(c)
    acc_k[...] = jnp.zeros_like(acc_k)
    acc_v[...] = jnp.zeros_like(acc_v)
    acc_q[...] = jnp.zeros_like(acc_q)
    for d, (o, other) in enumerate(((left, right), (right, left))):
        at = xg.at[0, o, pl.ds(half * (1 - d), half)]
        remote(at, at, own_send.at[d], first_recv.at[d], other).wait_recv()
    start(forward(0))
    start(own(1))
    for d, (o, other) in enumerate(((left, right), (right, left))):
        at = xg.at[0, o, pl.ds(half * d, half)]
        remote(at, at, own_send.at[d], late_recv.at[d], other).wait_recv()
    for c in range(2, AHEAD):
        start(own(c))

    def step(c, _):
        slot = lax.rem(c, 2)

        @pl.when(c + 1 < nk)
        def _():
            start(fetch(c + 1))
            received(arrival(c + 1))
            start(forward(c + 1))

        @pl.when(c + AHEAD < nk)
        def _():
            start(own(c + AHEAD))

        @pl.when(c + AHEAD + 1 < nk)
        def _():
            norm(c + AHEAD + 1)

        received(far(c))
        start([second(c)])
        pltpu.make_async_copy(ws.at[slot], ws.at[slot], wsem.at[slot]).wait()
        a = xg[c].reshape(n * rows, kc)
        b = xg[c, :, :half, :].reshape(n * half, kc)
        for i in range(0, cols, WIDE):
            acc_k[:, i : i + WIDE] += dot(a, ws[slot, 0, :, i : i + WIDE])
        for i in range(0, cols, WIDE):
            acc_v[:, i : i + WIDE] += dot(a, ws[slot, 1, :, i : i + WIDE])
        for i in range(0, cols, WIDE):
            acc_q[:, i : i + WIDE] += dot(b, ws[slot, 2, :, i : i + WIDE])
        return 0

    lax.fori_loop(0, nk, step, 0)

    group = 4 * HEAD

    def out(g):
        here = pl.ds(pl.multiple_of(g * group, group), group)
        return [pltpu.make_async_copy(ws.at[0, 0, :, here], k_out.at[:, here], osem.at[0, g]),
                pltpu.make_async_copy(ws.at[0, 1, :, here], v_out.at[:, here], osem.at[1, g]),
                pltpu.make_async_copy(ws.at[0, 2, pl.ds(0, n * half), here], q_out.at[:, here], osem.at[2, g])]

    def finish(g, _):
        here = pl.ds(pl.multiple_of(g * group, group), group)
        cos, sin = cos_ref[...].reshape(n * rows, HEAD), sin_ref[...].reshape(n * rows, HEAD)
        cos_q, sin_q = cos_ref[:, :half, :].reshape(n * half, HEAD), sin_ref[:, :half, :].reshape(n * half, HEAD)
        ws[0, 1, :, here] = acc_v[:, here].astype(BF16)
        for h in range(group // HEAD):
            at = pl.ds(pl.multiple_of(g * group + h * HEAD, HEAD), HEAD)
            ws[0, 0, :, at] = turn(acc_k[:, at], cos, sin)
            ws[0, 2, : n * half, at] = turn(acc_q[:, at], cos_q, sin_q)
        start(out(g))
        return 0

    lax.fori_loop(0, cols // group, finish, 0)
    pltpu.make_async_copy(xg.at[:, :, pl.ds(half, half), :], xb_out, xsem).wait()
    for d, other in enumerate((right, left)):
        at = xg.at[:, me]
        remote(at, at, own_send.at[d], first_recv.at[d], other).wait_send()
        at = xg.at[:, me, pl.ds(0, half)]
        remote(at, at, fwd_send.at[d], first_recv.at[d], other).wait_send()

    def drain(g, _):
        for copy in out(g):
            copy.wait()
        return 0

    lax.fori_loop(0, cols // group, drain, 0)


def attend_scatter(n, x_ref, q_ref, k_ref, v_ref, xb_ref, cos_ref, sin_ref, wq_ref, wo_ref, y_ref,
                   qs, ks, vs, att, xb, ring, acc, opp_b, out_r, out_l, add_r, add_l, own, half_l, half_r, full_l, full_r, xy,
                   rsem, insem, xbsem, xysem, ysem, hs_sem, hr_sem, fs_sem, fr_sem, free_r, free_l):
    me, right, left, opp = neighbours(n)
    width = wo_ref.shape[1]
    cols = wq_ref.shape[1]
    nt = width // TILE
    half = x_ref.shape[0] // 2
    part = half // 2
    parts = width // cols
    nq = (cols // TILE) * parts
    nkc, kc = xb_ref.shape[0], xb_ref.shape[3]
    group = 4 * HEAD
    tokens = k_ref.shape[0]

    def start(copies):
        for copy in copies:
            copy.start()

    def tile(t):
        return pl.ds(pl.multiple_of(t * TILE, TILE), TILE)

    def wo_tile(t, slot):
        return pltpu.make_async_copy(wo_ref.at[:, tile(t)], ring.at[slot], rsem.at[slot])

    def wq_tile(u, slot):
        p, j = lax.rem(u, parts), lax.div(u, parts)
        return pltpu.make_async_copy(wq_ref.at[pl.ds(pl.multiple_of(p * cols, cols), cols), tile(j)], ring.at[slot], rsem.at[slot])

    def fetch(u):
        slot = lax.rem(u, SLOTS)

        @pl.when(u < nt)
        def _():
            wo_tile(u, slot).start()

        @pl.when((u >= nt) & (u < nt + nq))
        def _():
            wq_tile(u - nt, slot).start()

        @pl.when((u >= nt + nq) & (u < 2 * nt + nq))
        def _():
            wo_tile(u - nt - nq, slot).start()

    def arrived(u):
        slot = lax.rem(u, SLOTS)
        wo_tile(0, slot).wait()
        return slot

    def inputs(g):
        here = pl.ds(pl.multiple_of(g * group, group), group)
        return [pltpu.make_async_copy(q_ref.at[:, here], qs.at[:, here], insem.at[0, g]),
                pltpu.make_async_copy(k_ref.at[:, here], ks.at[:, here], insem.at[1, g]),
                pltpu.make_async_copy(v_ref.at[:, here], vs.at[:, here], insem.at[2, g])]

    def rows_b(c):
        per = cols // kc
        return pltpu.make_async_copy(xb_ref.at[c], xb.at[lax.div(c, per), :, :, pl.ds(pl.multiple_of(lax.rem(c, per) * kc, kc), kc)], xbsem)

    def residual(h):
        return pltpu.make_async_copy(x_ref.at[pl.ds(h * half, half), :], xy.at[h], xysem.at[h])

    def result(h, t):
        return pltpu.make_async_copy(xy.at[h, :, tile(t)], y_ref.at[pl.ds(h * half, half), tile(t)], ysem.at[h])

    def halves(t):
        return [remote(opp_b.at[t, pl.ds(0, part)], half_l.at[t], hs_sem.at[0], hr_sem.at[t], right),
                remote(opp_b.at[t, pl.ds(part, part)], half_r.at[t], hs_sem.at[1], hr_sem.at[t], left)]

    def blocks(t):
        return [remote(out_r.at[t], full_l.at[t], fs_sem.at[0], fr_sem.at[t], right),
                remote(out_l.at[t], full_r.at[t], fs_sem.at[1], fr_sem.at[t], left)]

    def received(pair, sem):
        remote(pair, pair, hs_sem.at[0], sem, right).wait_recv()

    def attention(h, heads_ready):
        scale = HEAD**-0.5 * LOG2E

        def heads(g, _):
            heads_ready(g)
            for i in range(group // HEAD):
                at = pl.ds(pl.multiple_of(g * group + i * HEAD, HEAD), HEAD)
                for s in range(n // 2):
                    seen = (s + 1) * (tokens // (n // 2))
                    q = qs[pl.ds(s * 2 * half, 2 * half), at]
                    score = lax.dot_general(q, ks[:seen, at], (((1,), (1,)), ((), ())), preferred_element_type=F32)
                    row = lax.broadcasted_iota(jnp.int32, score.shape, 0)
                    place = (2 * s) * 2 * half + h * half + row + jnp.where(row >= half, half, 0)
                    score = jnp.where(lax.broadcasted_iota(jnp.int32, score.shape, 1) <= place, score, HIDDEN)
                    top = score.max(-1, keepdims=True)
                    weight = jnp.exp2((score - top) * scale)
                    got = dot(weight.astype(BF16), jnp.concatenate([vs[:seen, at], jnp.ones((seen, HEAD), BF16)], 1))
                    o = (got[:, :HEAD] / got[:, HEAD:]).astype(BF16)
                    for j in range(2):
                        att[lax.rem(2 * s + j + n - me, n), :, at] = o[j * half : (j + 1) * half]
            return 0

        lax.fori_loop(0, cols // group, heads, 0)

    def term(t, slot):
        got = dot(att[...].reshape(n * half, cols), ring[slot])
        own[t] = got[:half]
        add_r[t] = got[half : half + part]
        out_r[t, part:] = got[half + part : 2 * half].astype(BF16)
        opp_b[t] = got[2 * half : 3 * half].astype(BF16)
        out_l[t, :part] = got[3 * half : 3 * half + part].astype(BF16)
        add_l[t] = got[3 * half + part :]

    def add(t):
        received(opp_b.at[t], hr_sem.at[t])
        out_r[t, :part] = (add_r[t] + half_l[t].astype(F32)).astype(BF16)
        out_l[t, part:] = (add_l[t] + half_r[t].astype(F32)).astype(BF16)

    def close(h, t):
        received(out_r.at[pl.ds(0, 2)], fr_sem.at[t])
        here = tile(t)
        xy[h, :, here] = (xy[h, :, here].astype(F32) + (own[t] + full_l[t].astype(F32) + full_r[t].astype(F32))).astype(BF16)
        result(h, t).start()

    def serve(h, i):
        @pl.when((i >= 3) & (i - 3 < nt))
        def _():
            start(blocks(i - 3))

        @pl.when((i >= 2) & (i - 2 < nt))
        def _():
            add(i - 2)

        @pl.when((i >= LAG) & (i - LAG < nt))
        def _():
            close(h, i - LAG)

    def project(h, first):
        def pair(i, _):
            fetch(first + 2 * i + SLOTS - 2)
            fetch(first + 2 * i + SLOTS - 1)

            @pl.when(i >= 1)
            def _():
                start(halves(2 * i - 2))
                start(halves(2 * i - 1))

            serve(h, i)
            slots = [arrived(first + 2 * i + j) for j in range(2)]
            for j in range(2):
                term(2 * i + j, slots[j])
            return 0

        lax.fori_loop(0, nt // 2, pair, 0)
        start(halves(nt - 2))
        start(halves(nt - 1))

    def drain(h, i):
        added, sent = min(i - 2, nt), min(i - 3, nt)

        def rest(t, _):
            @pl.when(t >= added)
            def _():
                add(t)

            @pl.when(t - 1 >= sent)
            def _():
                start(blocks(t - 1))
            return 0

        if sent < nt:
            lax.fori_loop(sent, nt, rest, 0)
            start(blocks(nt - 1))

    def finish(h, i):
        closed = min(i - LAG, nt)

        def last(t, _):
            close(h, t)
            return 0

        lax.fori_loop(closed, nt, last, 0)

        for d, (a, b, other) in enumerate(((half_l, out_r, right), (half_r, out_l, left))):
            remote(a, a, hs_sem.at[d], hr_sem.at[0], other).wait_send()
            remote(b, b, fs_sem.at[d], fr_sem.at[0], other).wait_send()

    greeted = greet(right, left)

    def begin(g, _):
        start(inputs(g))
        return 0

    lax.fori_loop(0, cols // group, begin, 0)

    for u in range(SLOTS - 2):
        wo_tile(u, u).start()

    def begin_b(c, _):
        rows_b(c).start()
        return 0

    lax.fori_loop(0, nkc, begin_b, 0)
    for h in range(2):
        residual(h).start()

    def ready(g):
        for copy in inputs(g):
            copy.wait()

    attention(0, ready)
    for h in range(2):
        residual(h).wait()
    greeted()
    project(0, 0)

    pltpu.make_async_copy(xb, xb, xbsem).wait()

    def queries(j, _):
        for p in range(0, parts, 2):
            u = nt + j * parts + p
            fetch(u + SLOTS - 2)
            fetch(u + SLOTS - 1)
            serve(0, lax.div(u, 2))
            slots = [arrived(u + i) for i in range(2)]
            got = dot(xb[p].reshape(n * half, cols), ring[slots[0]]) + dot(xb[p + 1].reshape(n * half, cols), ring[slots[1]])
            acc[...] = got if p == 0 else acc[...] + got
        for i in range(TILE // HEAD):
            at = pl.ds(pl.multiple_of(j * TILE + i * HEAD, HEAD), HEAD)
            qs[:, at] = turn(acc[:, i * HEAD : (i + 1) * HEAD], cos_ref[...], sin_ref[...])
        return 0

    lax.fori_loop(0, cols // TILE, queries, 0)
    drain(0, (nt + nq) // 2)
    attention(1, lambda g: None)
    finish(0, (nt + nq) // 2)
    pl.semaphore_signal(free_r, inc=1, device_id={"tp": left}, device_id_type=MESH)
    pl.semaphore_signal(free_l, inc=1, device_id={"tp": right}, device_id_type=MESH)
    pl.semaphore_wait(free_r, 1)
    pl.semaphore_wait(free_l, 1)
    project(1, nt + nq)
    drain(1, nt // 2)
    finish(1, nt // 2)

    for h in range(2):
        pltpu.make_async_copy(xy.at[h], y_ref.at[pl.ds(h * half, half), :], ysem.at[h]).wait()


LAG = 7


def tables(tokens):
    i = HEAD // 2
    angle = np.arange(tokens, dtype=np.float32)[:, None] * np.power(np.float32(THETA), -np.arange(i, dtype=np.float32) / np.float32(i))
    cos, sin = np.cos(angle).astype(np.float32), np.sin(angle).astype(np.float32)
    return np.concatenate([cos, cos], 1), np.concatenate([-sin, sin], 1)


def solution(mesh):
    n = mesh.shape["tp"]
    anywhere = pl.BlockSpec(memory_space=pl.ANY)
    vmem = pl.BlockSpec(memory_space=pltpu.VMEM)
    dma = pltpu.SemaphoreType.DMA

    def first(x, gain, wk, wv, wq, cos, sin):
        rows, width = x.shape
        cols, nk, half = wk.shape[1], x.shape[1] // CHUNK, rows // 2
        return pl.pallas_call(
            functools.partial(gather_project, n),
            in_specs=[vmem] * 4 + [anywhere] * 3,
            out_specs=[anywhere] * 4,
            out_shape=[jax.ShapeDtypeStruct((n * rows, cols), BF16), jax.ShapeDtypeStruct((n * rows, cols), BF16),
                       jax.ShapeDtypeStruct((n * half, cols), BF16), jax.ShapeDtypeStruct((nk, n, half, CHUNK), BF16)],
            scratch_shapes=[
                pltpu.VMEM((nk, n, rows, CHUNK), BF16),
                pltpu.VMEM((n * rows, cols), F32), pltpu.VMEM((n * rows, cols), F32), pltpu.VMEM((n * half, cols), F32),
                pltpu.VMEM((2, 3, CHUNK, cols), BF16), pltpu.VMEM((rows, 128), F32),
                dma((2,)), dma((2,)), dma((2,)), dma((2,)), dma((nk,)), dma((2,)), dma((nk,)), dma, dma((3, cols // (4 * HEAD)))],
            compiler_params=pltpu.CompilerParams(collective_id=0, has_side_effects=True, vmem_limit_bytes=LIMIT),
            name="gather_project",
        )(x, gain, cos.reshape(n, rows, HEAD), sin.reshape(n, rows, HEAD), wk, wv, wq)

    def then(x, q, k, v, xb, cos, sin, wq, wo):
        rows, width = x.shape
        cols, nt, half = wq.shape[1], x.shape[1] // TILE, rows // 2
        nk, part = xb.shape[0], half // 2
        cos, sin = (a.reshape(n, 2, half, HEAD)[:, 1].reshape(n * half, HEAD) for a in (cos, sin))
        return pl.pallas_call(
            functools.partial(attend_scatter, n),
            in_specs=[anywhere] * 5 + [vmem] * 2 + [anywhere] * 2,
            out_specs=anywhere,
            out_shape=jax.ShapeDtypeStruct((rows, width), BF16),
            scratch_shapes=[
                pltpu.VMEM((n * half, cols), BF16), pltpu.VMEM((n * rows, cols), BF16), pltpu.VMEM((n * rows, cols), BF16),
                pltpu.VMEM((n, half, cols), BF16), pltpu.VMEM((width // cols, n, half, cols), BF16),
                pltpu.VMEM((SLOTS, cols, TILE), BF16), pltpu.VMEM((n * half, TILE), F32),
                pltpu.VMEM((nt, half, TILE), BF16), pltpu.VMEM((nt, half, TILE), BF16), pltpu.VMEM((nt, half, TILE), BF16),
                pltpu.VMEM((nt, part, TILE), F32), pltpu.VMEM((nt, part, TILE), F32), pltpu.VMEM((nt, half, TILE), F32),
                pltpu.VMEM((nt, part, TILE), BF16), pltpu.VMEM((nt, part, TILE), BF16),
                pltpu.VMEM((nt, half, TILE), BF16), pltpu.VMEM((nt, half, TILE), BF16),
                pltpu.VMEM((2, half, width), BF16),
                dma((SLOTS,)), dma((3, cols // (4 * HEAD))), dma, dma((2,)), dma((2,)),
                dma((2,)), dma((nt,)), dma((2,)), dma((nt,)),
                pltpu.SemaphoreType.REGULAR, pltpu.SemaphoreType.REGULAR],
            compiler_params=pltpu.CompilerParams(collective_id=1, has_side_effects=True, vmem_limit_bytes=LIMIT),
            name="attend_scatter",
        )(x, q, k, v, xb, cos, sin, wq, wo)

    def step(x, gain, wq, wk, wv, wo):
        cos, sin = tables(n * x.shape[0])
        k, v, q, xb = first(x, gain, wk, wv, wq, cos, sin)
        return then(x, q, k, v, xb, cos, sin, wq, wo)

    tokens, columns = P(("dp", "tp"), None), P(None, "tp")
    return jax.shard_map(
        step,
        mesh=mesh,
        in_specs=(tokens, P(None), columns, columns, columns, P("tp", None)),
        out_specs=tokens,
        check_vma=False,
    )
```

```python
import functools

import jax
import jax.numpy as jnp
import numpy as np
from jax import lax
from jax.experimental import pallas as pl
from jax.experimental.pallas import tpu as pltpu
from jax.sharding import PartitionSpec as P

HEAD = 128
THETA = 10000
EPS = 1e-6
LOG2E = 1.4426950408889634
HIDDEN = -2e30
CHUNK = 512
WIDE = 512
TILE = 512
AHEAD = 3
SLOTS = 5
LIMIT = 63 * 2**20 + 900 * 2**10
MESH = pl.DeviceIdType.MESH
F32, BF16 = jnp.float32, jnp.bfloat16


def dot(a, b):
    return jnp.dot(a, b, preferred_element_type=F32)


def neighbours(n):
    me = lax.axis_index("tp")
    return me, lax.rem(me + 1, n), lax.rem(me + n - 1, n), lax.rem(me + 2, n)


def greet(right, left):
    barrier = pltpu.get_barrier_semaphore()
    for other in (right, left):
        pl.semaphore_signal(barrier, inc=1, device_id={"tp": other}, device_id_type=MESH)
    return lambda: pl.semaphore_wait(barrier, 2)


def remote(src, dst, send, recv, other):
    return pltpu.make_async_remote_copy(src_ref=src, dst_ref=dst, send_sem=send, recv_sem=recv, device_id={"tp": other}, device_id_type=MESH)


def turn(t, cos, sin):
    t = t.astype(BF16).astype(F32)
    return (t * cos + pltpu.roll(t, HEAD // 2, 1) * sin).astype(BF16)


def gather_project(n, x_ref, gain_ref, cos_ref, sin_ref, wk_ref, wv_ref, wq_ref, k_out, v_out, q_out, xb_out,
                   xg, acc_k, acc_v, acc_q, ws, scale_s, wsem, first_recv, late_recv, own_send, own_recv, fwd_send, fwd_recv, xsem, osem):
    me, right, left, opp = neighbours(n)
    rows, width = x_ref.shape
    nk, kc, cols = width // CHUNK, CHUNK, wk_ref.shape[1]
    half = rows // 2
    weights = (wk_ref, wv_ref, wq_ref)

    def fetch(c):
        slot = lax.rem(c, 2)
        return [pltpu.make_async_copy(w.at[pl.ds(pl.multiple_of(c * kc, kc), kc), :], ws.at[slot, i], wsem.at[slot])
                for i, w in enumerate(weights)]

    def own(c):
        return [remote(xg.at[c, me], xg.at[c, me], own_send.at[d], own_recv.at[c], other) for d, other in enumerate((right, left))]

    def arrival(c):
        both = xg.at[c, pl.ds(0, 2)]
        return [remote(both, both, own_send.at[0], own_recv.at[c], right)]

    def forward(c):
        a, b = xg.at[c, left, pl.ds(half, half)], xg.at[c, right, pl.ds(0, half)]
        return [remote(a, a, fwd_send.at[0], fwd_recv.at[c], right), remote(b, b, fwd_send.at[1], fwd_recv.at[c], left)]

    def far(c):
        return [remote(xg.at[c, opp], xg.at[c, opp], fwd_send.at[0], fwd_recv.at[c], right)]

    def second(c):
        return pltpu.make_async_copy(xg.at[c, :, pl.ds(half, half), :], xb_out.at[c], xsem)

    def norm(c):
        here = pl.ds(pl.multiple_of(c * kc, kc), kc)
        wide = x_ref[:, here].astype(F32)
        xg[c, me] = (wide * scale_s[:, :1] * gain_ref[here].astype(F32)[None]).astype(BF16)

    def start(copies):
        for copy in copies:
            copy.start()

    def received(copies):
        for copy in copies:
            copy.wait_recv()

    greeted = greet(right, left)
    start(fetch(0))

    def squares(c, total):
        wide = x_ref[:, pl.ds(pl.multiple_of(c * kc, kc), kc)].astype(F32)
        wide = wide * wide
        for i in range(0, kc, 128):
            total = total + wide[:, i : i + 128]
        return total

    total = lax.fori_loop(0, nk, squares, jnp.zeros((rows, 128), F32))
    scale_s[...] = jnp.broadcast_to(lax.rsqrt(total.sum(-1, keepdims=True) * (1 / width) + EPS), (rows, 128))
    norm(0)
    norm(1)
    greeted()
    for there, sems in ((0, first_recv), (1, late_recv)):
        for d, other in enumerate((right, left)):
            at = xg.at[0, me, pl.ds(half * ((there + d + 1) % 2), half)]
            remote(at, at, own_send.at[d], sems.at[d], other).start()
    for c in range(2, AHEAD + 1):
        norm(c)
    acc_k[...] = jnp.zeros_like(acc_k)
    acc_v[...] = jnp.zeros_like(acc_v)
    acc_q[...] = jnp.zeros_like(acc_q)
    for d, (o, other) in enumerate(((left, right), (right, left))):
        at = xg.at[0, o, pl.ds(half * (1 - d), half)]
        remote(at, at, own_send.at[d], first_recv.at[d], other).wait_recv()
    start(forward(0))
    start(own(1))
    for d, (o, other) in enumerate(((left, right), (right, left))):
        at = xg.at[0, o, pl.ds(half * d, half)]
        remote(at, at, own_send.at[d], late_recv.at[d], other).wait_recv()
    for c in range(2, AHEAD):
        start(own(c))

    def step(c, _):
        slot = lax.rem(c, 2)

        @pl.when(c + 1 < nk)
        def _():
            start(fetch(c + 1))
            received(arrival(c + 1))
            start(forward(c + 1))

        @pl.when(c + AHEAD < nk)
        def _():
            start(own(c + AHEAD))

        @pl.when(c + AHEAD + 1 < nk)
        def _():
            norm(c + AHEAD + 1)

        received(far(c))
        start([second(c)])
        pltpu.make_async_copy(ws.at[slot], ws.at[slot], wsem.at[slot]).wait()
        a = xg[c].reshape(n * rows, kc)
        b = xg[c, :, :half, :].reshape(n * half, kc)
        for i in range(0, cols, WIDE):
            acc_k[:, i : i + WIDE] += dot(a, ws[slot, 0, :, i : i + WIDE])
        for i in range(0, cols, WIDE):
            acc_v[:, i : i + WIDE] += dot(a, ws[slot, 1, :, i : i + WIDE])
        for i in range(0, cols, WIDE):
            acc_q[:, i : i + WIDE] += dot(b, ws[slot, 2, :, i : i + WIDE])
        return 0

    lax.fori_loop(0, nk, step, 0)

    group = 4 * HEAD

    def out(g):
        here = pl.ds(pl.multiple_of(g * group, group), group)
        return [pltpu.make_async_copy(ws.at[0, 0, :, here], k_out.at[:, here], osem.at[0, g]),
                pltpu.make_async_copy(ws.at[0, 1, :, here], v_out.at[:, here], osem.at[1, g]),
                pltpu.make_async_copy(ws.at[0, 2, pl.ds(0, n * half), here], q_out.at[:, here], osem.at[2, g])]

    def finish(g, _):
        here = pl.ds(pl.multiple_of(g * group, group), group)
        cos, sin = cos_ref[...].reshape(n * rows, HEAD), sin_ref[...].reshape(n * rows, HEAD)
        cos_q, sin_q = cos_ref[:, :half, :].reshape(n * half, HEAD), sin_ref[:, :half, :].reshape(n * half, HEAD)
        ws[0, 1, :, here] = acc_v[:, here].astype(BF16)
        for h in range(group // HEAD):
            at = pl.ds(pl.multiple_of(g * group + h * HEAD, HEAD), HEAD)
            ws[0, 0, :, at] = turn(acc_k[:, at], cos, sin)
            ws[0, 2, : n * half, at] = turn(acc_q[:, at], cos_q, sin_q)
        start(out(g))
        return 0

    lax.fori_loop(0, cols // group, finish, 0)
    pltpu.make_async_copy(xg.at[:, :, pl.ds(half, half), :], xb_out, xsem).wait()
    for d, other in enumerate((right, left)):
        at = xg.at[:, me]
        remote(at, at, own_send.at[d], first_recv.at[d], other).wait_send()
        at = xg.at[:, me, pl.ds(0, half)]
        remote(at, at, fwd_send.at[d], first_recv.at[d], other).wait_send()

    def drain(g, _):
        for copy in out(g):
            copy.wait()
        return 0

    lax.fori_loop(0, cols // group, drain, 0)


def attend_scatter(n, x_ref, q_ref, k_ref, v_ref, xb_ref, cos_ref, sin_ref, wq_ref, wo_ref, y_ref,
                   qs, ks, vs, att, xb, ring, acc, opp_b, out_r, out_l, add_r, add_l, own, half_l, half_r, full_l, full_r, xy,
                   rsem, insem, xbsem, xysem, ysem, hs_sem, hr_sem, fs_sem, fr_sem, free_r, free_l):
    me, right, left, opp = neighbours(n)
    width = wo_ref.shape[1]
    cols = wq_ref.shape[1]
    nt = width // TILE
    half = x_ref.shape[0] // 2
    part = half // 2
    parts = width // cols
    nq = (cols // TILE) * parts
    nkc, kc = xb_ref.shape[0], xb_ref.shape[3]
    group = 4 * HEAD
    tokens = k_ref.shape[0]

    def start(copies):
        for copy in copies:
            copy.start()

    def tile(t):
        return pl.ds(pl.multiple_of(t * TILE, TILE), TILE)

    def wo_tile(t, slot):
        return pltpu.make_async_copy(wo_ref.at[:, tile(t)], ring.at[slot], rsem.at[slot])

    def wq_tile(u, slot):
        p, j = lax.rem(u, parts), lax.div(u, parts)
        return pltpu.make_async_copy(wq_ref.at[pl.ds(pl.multiple_of(p * cols, cols), cols), tile(j)], ring.at[slot], rsem.at[slot])

    def fetch(u):
        slot = lax.rem(u, SLOTS)

        @pl.when(u < nt)
        def _():
            wo_tile(u, slot).start()

        @pl.when((u >= nt) & (u < nt + nq))
        def _():
            wq_tile(u - nt, slot).start()

        @pl.when((u >= nt + nq) & (u < 2 * nt + nq))
        def _():
            wo_tile(u - nt - nq, slot).start()

    def arrived(u):
        slot = lax.rem(u, SLOTS)
        wo_tile(0, slot).wait()
        return slot

    def inputs(g):
        here = pl.ds(pl.multiple_of(g * group, group), group)
        return [pltpu.make_async_copy(q_ref.at[:, here], qs.at[:, here], insem.at[0, g]),
                pltpu.make_async_copy(k_ref.at[:, here], ks.at[:, here], insem.at[1, g]),
                pltpu.make_async_copy(v_ref.at[:, here], vs.at[:, here], insem.at[2, g])]

    def rows_b(c):
        per = cols // kc
        return pltpu.make_async_copy(xb_ref.at[c], xb.at[lax.div(c, per), :, :, pl.ds(pl.multiple_of(lax.rem(c, per) * kc, kc), kc)], xbsem)

    def residual(h):
        return pltpu.make_async_copy(x_ref.at[pl.ds(h * half, half), :], xy.at[h], xysem.at[h])

    def result(h, t):
        return pltpu.make_async_copy(xy.at[h, :, tile(t)], y_ref.at[pl.ds(h * half, half), tile(t)], ysem.at[h])

    def halves(t):
        return [remote(opp_b.at[t, pl.ds(0, part)], half_l.at[t], hs_sem.at[0], hr_sem.at[t], right),
                remote(opp_b.at[t, pl.ds(part, part)], half_r.at[t], hs_sem.at[1], hr_sem.at[t], left)]

    def blocks(t):
        return [remote(out_r.at[t], full_l.at[t], fs_sem.at[0], fr_sem.at[t], right),
                remote(out_l.at[t], full_r.at[t], fs_sem.at[1], fr_sem.at[t], left)]

    def received(pair, sem):
        remote(pair, pair, hs_sem.at[0], sem, right).wait_recv()

    def attention(h, heads_ready):
        scale = HEAD**-0.5 * LOG2E

        def heads(g, _):
            heads_ready(g)
            for i in range(group // HEAD):
                at = pl.ds(pl.multiple_of(g * group + i * HEAD, HEAD), HEAD)
                for s in range(n // 2):
                    seen = (s + 1) * (tokens // (n // 2))
                    q = qs[pl.ds(s * 2 * half, 2 * half), at]
                    score = lax.dot_general(q, ks[:seen, at], (((1,), (1,)), ((), ())), preferred_element_type=F32)
                    row = lax.broadcasted_iota(jnp.int32, score.shape, 0)
                    place = (2 * s) * 2 * half + h * half + row + jnp.where(row >= half, half, 0)
                    score = jnp.where(lax.broadcasted_iota(jnp.int32, score.shape, 1) <= place, score, HIDDEN)
                    top = score.max(-1, keepdims=True)
                    weight = jnp.exp2((score - top) * scale)
                    got = dot(weight.astype(BF16), jnp.concatenate([vs[:seen, at], jnp.ones((seen, HEAD), BF16)], 1))
                    o = (got[:, :HEAD] / got[:, HEAD:]).astype(BF16)
                    for j in range(2):
                        att[lax.rem(2 * s + j + n - me, n), :, at] = o[j * half : (j + 1) * half]
            return 0

        lax.fori_loop(0, cols // group, heads, 0)

    def term(t, slot):
        got = dot(att[...].reshape(n * half, cols), ring[slot])
        own[t] = got[:half]
        add_r[t] = got[half : half + part]
        out_r[t, part:] = got[half + part : 2 * half].astype(BF16)
        opp_b[t] = got[2 * half : 3 * half].astype(BF16)
        out_l[t, :part] = got[3 * half : 3 * half + part].astype(BF16)
        add_l[t] = got[3 * half + part :]

    def add(t):
        received(opp_b.at[t], hr_sem.at[t])
        out_r[t, :part] = (add_r[t] + half_l[t].astype(F32)).astype(BF16)
        out_l[t, part:] = (add_l[t] + half_r[t].astype(F32)).astype(BF16)

    def close(h, t):
        received(out_r.at[pl.ds(0, 2)], fr_sem.at[t])
        here = tile(t)
        xy[h, :, here] = (xy[h, :, here].astype(F32) + (own[t] + full_l[t].astype(F32) + full_r[t].astype(F32))).astype(BF16)
        result(h, t).start()

    def serve(h, i):
        @pl.when((i >= 2) & (i - 2 < nt))
        def _():
            start(blocks(i - 2))

        @pl.when((i >= LAG) & (i - LAG < nt))
        def _():
            close(h, i - LAG)

    def follow(i):
        @pl.when((i >= 1) & (i - 1 < nt))
        def _():
            add(i - 1)

    def project(h, first):
        def pair(i, _):
            fetch(first + 2 * i + SLOTS - 2)
            fetch(first + 2 * i + SLOTS - 1)

            @pl.when(i >= 1)
            def _():
                start(halves(2 * i - 2))
                start(halves(2 * i - 1))

            serve(h, i)
            slots = [arrived(first + 2 * i + j) for j in range(2)]
            for j in range(2):
                term(2 * i + j, slots[j])
            follow(i)
            return 0

        lax.fori_loop(0, nt // 2, pair, 0)
        start(halves(nt - 2))
        start(halves(nt - 1))

    def drain(h, i):
        added, sent = min(i - 1, nt), min(i - 2, nt)

        def rest(t, _):
            @pl.when(t >= added)
            def _():
                add(t)

            @pl.when(t - 1 >= sent)
            def _():
                start(blocks(t - 1))
            return 0

        if sent < nt:
            lax.fori_loop(sent, nt, rest, 0)
            start(blocks(nt - 1))

    def finish(h, i):
        closed = min(i - LAG, nt)

        def last(t, _):
            close(h, t)
            return 0

        lax.fori_loop(closed, nt, last, 0)

        for d, (a, b, other) in enumerate(((half_l, out_r, right), (half_r, out_l, left))):
            remote(a, a, hs_sem.at[d], hr_sem.at[0], other).wait_send()
            remote(b, b, fs_sem.at[d], fr_sem.at[0], other).wait_send()

    greeted = greet(right, left)

    def begin(g, _):
        start(inputs(g))
        return 0

    lax.fori_loop(0, cols // group, begin, 0)

    for u in range(SLOTS - 2):
        wo_tile(u, u).start()

    def begin_b(c, _):
        rows_b(c).start()
        return 0

    lax.fori_loop(0, nkc, begin_b, 0)
    for h in range(2):
        residual(h).start()

    def ready(g):
        for copy in inputs(g):
            copy.wait()

    attention(0, ready)
    for h in range(2):
        residual(h).wait()
    greeted()
    project(0, 0)

    pltpu.make_async_copy(xb, xb, xbsem).wait()

    def queries(j, _):
        for p in range(0, parts, 2):
            u = nt + j * parts + p
            fetch(u + SLOTS - 2)
            fetch(u + SLOTS - 1)
            serve(0, lax.div(u, 2))
            slots = [arrived(u + i) for i in range(2)]
            got = dot(xb[p].reshape(n * half, cols), ring[slots[0]]) + dot(xb[p + 1].reshape(n * half, cols), ring[slots[1]])
            acc[...] = got if p == 0 else acc[...] + got
            follow(lax.div(u, 2))
        for i in range(TILE // HEAD):
            at = pl.ds(pl.multiple_of(j * TILE + i * HEAD, HEAD), HEAD)
            qs[:, at] = turn(acc[:, i * HEAD : (i + 1) * HEAD], cos_ref[...], sin_ref[...])
        return 0

    lax.fori_loop(0, cols // TILE, queries, 0)
    drain(0, (nt + nq) // 2)
    attention(1, lambda g: None)
    finish(0, (nt + nq) // 2)
    pl.semaphore_signal(free_r, inc=1, device_id={"tp": left}, device_id_type=MESH)
    pl.semaphore_signal(free_l, inc=1, device_id={"tp": right}, device_id_type=MESH)
    pl.semaphore_wait(free_r, 1)
    pl.semaphore_wait(free_l, 1)
    project(1, nt + nq)
    drain(1, nt // 2)
    finish(1, nt // 2)

    for h in range(2):
        pltpu.make_async_copy(xy.at[h], y_ref.at[pl.ds(h * half, half), :], ysem.at[h]).wait()


LAG = 6


def tables(tokens):
    i = HEAD // 2
    angle = np.arange(tokens, dtype=np.float32)[:, None] * np.power(np.float32(THETA), -np.arange(i, dtype=np.float32) / np.float32(i))
    cos, sin = np.cos(angle).astype(np.float32), np.sin(angle).astype(np.float32)
    return np.concatenate([cos, cos], 1), np.concatenate([-sin, sin], 1)


def solution(mesh):
    n = mesh.shape["tp"]
    anywhere = pl.BlockSpec(memory_space=pl.ANY)
    vmem = pl.BlockSpec(memory_space=pltpu.VMEM)
    dma = pltpu.SemaphoreType.DMA

    def first(x, gain, wk, wv, wq, cos, sin):
        rows, width = x.shape
        cols, nk, half = wk.shape[1], x.shape[1] // CHUNK, rows // 2
        return pl.pallas_call(
            functools.partial(gather_project, n),
            in_specs=[vmem] * 4 + [anywhere] * 3,
            out_specs=[anywhere] * 4,
            out_shape=[jax.ShapeDtypeStruct((n * rows, cols), BF16), jax.ShapeDtypeStruct((n * rows, cols), BF16),
                       jax.ShapeDtypeStruct((n * half, cols), BF16), jax.ShapeDtypeStruct((nk, n, half, CHUNK), BF16)],
            scratch_shapes=[
                pltpu.VMEM((nk, n, rows, CHUNK), BF16),
                pltpu.VMEM((n * rows, cols), F32), pltpu.VMEM((n * rows, cols), F32), pltpu.VMEM((n * half, cols), F32),
                pltpu.VMEM((2, 3, CHUNK, cols), BF16), pltpu.VMEM((rows, 128), F32),
                dma((2,)), dma((2,)), dma((2,)), dma((2,)), dma((nk,)), dma((2,)), dma((nk,)), dma, dma((3, cols // (4 * HEAD)))],
            compiler_params=pltpu.CompilerParams(collective_id=0, has_side_effects=True, vmem_limit_bytes=LIMIT),
            name="gather_project",
        )(x, gain, cos.reshape(n, rows, HEAD), sin.reshape(n, rows, HEAD), wk, wv, wq)

    def then(x, q, k, v, xb, cos, sin, wq, wo):
        rows, width = x.shape
        cols, nt, half = wq.shape[1], x.shape[1] // TILE, rows // 2
        nk, part = xb.shape[0], half // 2
        cos, sin = (a.reshape(n, 2, half, HEAD)[:, 1].reshape(n * half, HEAD) for a in (cos, sin))
        return pl.pallas_call(
            functools.partial(attend_scatter, n),
            in_specs=[anywhere] * 5 + [vmem] * 2 + [anywhere] * 2,
            out_specs=anywhere,
            out_shape=jax.ShapeDtypeStruct((rows, width), BF16),
            scratch_shapes=[
                pltpu.VMEM((n * half, cols), BF16), pltpu.VMEM((n * rows, cols), BF16), pltpu.VMEM((n * rows, cols), BF16),
                pltpu.VMEM((n, half, cols), BF16), pltpu.VMEM((width // cols, n, half, cols), BF16),
                pltpu.VMEM((SLOTS, cols, TILE), BF16), pltpu.VMEM((n * half, TILE), F32),
                pltpu.VMEM((nt, half, TILE), BF16), pltpu.VMEM((nt, half, TILE), BF16), pltpu.VMEM((nt, half, TILE), BF16),
                pltpu.VMEM((nt, part, TILE), F32), pltpu.VMEM((nt, part, TILE), F32), pltpu.VMEM((nt, half, TILE), F32),
                pltpu.VMEM((nt, part, TILE), BF16), pltpu.VMEM((nt, part, TILE), BF16),
                pltpu.VMEM((nt, half, TILE), BF16), pltpu.VMEM((nt, half, TILE), BF16),
                pltpu.VMEM((2, half, width), BF16),
                dma((SLOTS,)), dma((3, cols // (4 * HEAD))), dma, dma((2,)), dma((2,)),
                dma((2,)), dma((nt,)), dma((2,)), dma((nt,)),
                pltpu.SemaphoreType.REGULAR, pltpu.SemaphoreType.REGULAR],
            compiler_params=pltpu.CompilerParams(collective_id=1, has_side_effects=True, vmem_limit_bytes=LIMIT),
            name="attend_scatter",
        )(x, q, k, v, xb, cos, sin, wq, wo)

    def step(x, gain, wq, wk, wv, wo):
        cos, sin = tables(n * x.shape[0])
        k, v, q, xb = first(x, gain, wk, wv, wq, cos, sin)
        return then(x, q, k, v, xb, cos, sin, wq, wo)

    tokens, columns = P(("dp", "tp"), None), P(None, "tp")
    return jax.shard_map(
        step,
        mesh=mesh,
        in_specs=(tokens, P(None), columns, columns, columns, P("tp", None)),
        out_specs=tokens,
        check_vma=False,
    )
```
